32 devices in a mesh: pool: 16 (over z, y, x), con: 2 (over core).
Axes of the slice: x: 2, y: 2, z: 4, core: 2. Of those that a mesh axis runs over, the one named last changes fastest.
Arguments:
- pool_feat: bfloat16 [8192, 64], P('pool'), may hold values from -5 to 5
- contract_feat: bfloat16 [8192, 64], P('con'), may hold values from -5 to 5
- supply: float32 [8192], P('pool'), may hold values from 0.3 to 4
- caps: int32 [8192], P('con'), may hold values from 1 to 16
- eligible: int32 [64, 64], P('pool', 'con'), may hold values from 0 to 1, as said below
- grad_log_pool: float32 [8192], P('pool'), may hold values from -48 to 48
- grad_log_contract: float32 [8192], P('con'), may hold values from -48 to 48
Outputs:
- pool_grad: float32 [8192, 64], P('pool')
- contract_grad: float32 [8192, 64], P('con')
The draws below stay inside these ranges and needn't reach their ends.
Inputs may be any that keep to these rules, and one draw needn't show every extreme that they name: `eligible`: values are 0 or 1; every row of tiles and every column of tiles holds at least one 1.
All inputs are finite; a program needn't handle non-finite values.
Results may differ from the reference program's by a relative error of at most 0.0026.
Values sent between devices are 32-bit elements; how exact they have to be, the bound alone decides.
A program may use at most 64 MiB of HBM per device.

```python
import math
import jax
import jax.numpy as jnp
from jax import lax

F = 64
TILE = 128
ITERS = 2
COLS_DEV = 4096
POOLS = 8192
CONTRACTS = 8192


def draw_eligible(key, part):
    row_tiles = POOLS // TILE
    col_tiles = CONTRACTS // TILE
    random_part = (jax.random.randint(key, (row_tiles, col_tiles), 0, 5) < 3).astype(jnp.int32)
    row_index = jnp.arange(row_tiles, dtype=jnp.int32)[:, None]
    col_index = jnp.arange(col_tiles, dtype=jnp.int32)[None, :]
    forced = jnp.logical_or(col_index % row_tiles == row_index, row_index % col_tiles == col_index)
    return jnp.maximum(random_part, forced.astype(jnp.int32))


def touch_ends(drawn, key, low, largest):
    longest = drawn.shape.index(max(drawn.shape))
    spots = []
    for shift in (0, 1):
        where = [jax.random.randint(jax.random.fold_in(key, axis), (), 0, length) for axis, length in enumerate(drawn.shape)]
        where[longest] = (where[longest] + shift) % drawn.shape[longest]
        spots.append(tuple(where))
    return drawn.at[spots[0]].set(low).at[spots[1]].set(largest)


def levels(rng, dims, split, least, largest):
    loudness, own = 1.0, jax.random.fold_in(rng, 6)
    for axis_at, blocks in split:
        draws = jnp.exp(jax.random.uniform(jax.random.fold_in(own, axis_at), (blocks,), jnp.float32, least / len(split), largest / len(split)))
        loudness = loudness * jnp.repeat(draws, dims[axis_at] // blocks).reshape([-1 if axis == axis_at else 1 for axis in range(len(dims))])
    return loudness


def bell_draw(rng, dims, spread, limit, shards=(), kind=jnp.bfloat16):
    level = levels(rng, dims, shards, -0.22, 0.18) if shards else 1.0
    drawn = jax.random.normal(rng, dims, jnp.float32) * spread * level
    return jnp.minimum(jnp.maximum(drawn, -limit), limit).astype(kind)


def setup_inputs(seed: int = 0) -> dict:
    arg_keys = jax.random.split(jax.random.key(seed), 8)
    pool_feat = bell_draw(arg_keys[0], (POOLS, F), 1.0, 5.0, ((0, 16),))
    contract_feat = bell_draw(arg_keys[1], (CONTRACTS, F), 1.0, 5.0, ((0, 2),))
    supply = jnp.clip(jnp.exp(math.log(4.0) - 2.5902671 * jax.random.uniform(arg_keys[2], (POOLS,), jnp.float32) ** levels(arg_keys[2], (POOLS,), ((0, 16),), -0.2, 0.2)), 0.3, 4.0)
    caps = touch_ends(jax.random.randint(arg_keys[3], (CONTRACTS,), 1, 17), jax.random.fold_in(arg_keys[3], 1), 1, 16).astype(jnp.int32)
    eligible = draw_eligible(jax.random.fold_in(arg_keys[7], 71), 0)
    grad_log_pool = bell_draw(arg_keys[5], (POOLS,), 8.0, 48.0, ((0, 16),), jnp.float32)
    grad_log_contract = bell_draw(arg_keys[6], (CONTRACTS,), 8.0, 48.0, ((0, 2),), jnp.float32)
    return dict(pool_feat=pool_feat, contract_feat=contract_feat, supply=supply, caps=caps, eligible=eligible, grad_log_pool=grad_log_pool, grad_log_contract=grad_log_contract)


HIGHEST_PRECISION = lax.Precision.HIGHEST


def kernel_tile(pool_feat, feat_block, mask_block):
    scores = jnp.dot(pool_feat, feat_block.T, preferred_element_type=jnp.float32) * 0.125
    values = jnp.exp(scores)
    row_count, col_count = values.shape
    shaped = values.reshape(row_count // TILE, TILE, col_count // TILE, TILE) * mask_block.astype(jnp.float32)[:, None, :, None]
    return shaped.reshape(row_count, col_count)


def reference(pool_feat, contract_feat, supply, caps, eligible, grad_log_pool, grad_log_contract):
    block_width = min(1024, COLS_DEV)
    blocks = CONTRACTS // block_width
    feat_blocks = contract_feat.reshape(blocks, block_width, F)
    mask_blocks = eligible.reshape(POOLS // TILE, blocks, block_width // TILE).transpose(1, 0, 2)
    demand = caps.astype(jnp.float32)

    def column_sums(weights):
        def per_block(entries):
            return jnp.dot(weights, kernel_tile(pool_feat, entries[0], entries[1]), precision=HIGHEST_PRECISION)
        return lax.map(per_block, (feat_blocks, mask_blocks)).reshape(CONTRACTS)

    def row_sums(weights):
        weight_blocks = weights.reshape(blocks, block_width)

        def per_block(summed, entries):
            kernel = kernel_tile(pool_feat, entries[0], entries[1])
            return summed + jnp.dot(kernel, entries[2], precision=HIGHEST_PRECISION), None
        summed, _ = lax.scan(per_block, jnp.zeros((POOLS,), jnp.float32), (feat_blocks, mask_blocks, weight_blocks))
        return summed

    pool_scale = jnp.ones((POOLS,), jnp.float32)
    earlier = []
    contract_scales = []
    row_results = []
    for iteration in range(ITERS):
        earlier.append(pool_scale)
        contract_scale = demand / column_sums(pool_scale)
        row_total = row_sums(contract_scale)
        pool_scale = supply / row_total
        contract_scales.append(contract_scale)
        row_results.append(row_total)

    row_adj = -grad_log_pool / row_results[-1]
    left_parts = []
    right_parts = []
    for iteration in reversed(range(ITERS)):
        summed = column_sums(row_adj)
        contract_scale = contract_scales[iteration]
        if iteration == ITERS - 1:
            col_adj = -(grad_log_contract / contract_scale + summed) * contract_scale * contract_scale / demand
        else:
            col_adj = -summed * contract_scale * contract_scale / demand
        left_parts += [row_adj, earlier[iteration]]
        right_parts += [contract_scale, col_adj]
        if iteration > 0:
            pool_adj = row_sums(col_adj)
            row_adj = -pool_adj * earlier[iteration] / row_results[iteration - 1]

    left_mat = jnp.stack(left_parts, axis=1)
    right_blocks = jnp.stack(right_parts, axis=1).reshape(blocks, block_width, 2 * ITERS)

    def final_block(carried, entries):
        kernel = kernel_tile(pool_feat, entries[0], entries[1])
        weights = jnp.dot(left_mat, entries[2].T, precision=HIGHEST_PRECISION)
        product = (kernel * weights).astype(jnp.bfloat16)
        carried = carried + jnp.dot(product, entries[0], preferred_element_type=jnp.float32) * 0.125
        column_part = lax.dot_general(product, pool_feat, (((0,), (0,)), ((), ())), preferred_element_type=jnp.float32) * 0.125
        return carried, column_part

    pool_grad, column_blocks = lax.scan(final_block, jnp.zeros((POOLS, F), jnp.float32), (feat_blocks, mask_blocks, right_blocks))
    return pool_grad, column_blocks.reshape(CONTRACTS, F)
```

```python
import functools
import math

import jax
import jax.numpy as jnp
from jax import lax
from jax.experimental import pallas as pl
from jax.experimental.pallas import tpu as pltpu
from jax.sharding import PartitionSpec as P

MESH = pl.DeviceIdType.MESH
F32 = jnp.float32
BF16 = jnp.bfloat16
INNER = 4
SCALE = 0.125
NN = (((1,), (0,)), ((), ()))
NT = (((1,), (1,)), ((), ()))
TN = (((0,), (0,)), ((), ()))


def dot(a, b, dims):
    return lax.dot_general(a, b, dims, preferred_element_type=F32)


def parts(x):
    high = x.astype(BF16).astype(F32)
    return high, x - high


def split_rows(x):
    high, low = parts(x)
    row = lax.broadcasted_iota(jnp.int32, (8, x.shape[1]), 0)
    return jnp.where(row == 0, high, jnp.where(row == 1, low, 0.0)).astype(BF16)


def fill_rows(ref, rows):
    for at, row in enumerate(rows):
        ref[at : at + 1, :] = row
    ref[len(rows) :, :] = jnp.zeros((ref.shape[0] - len(rows), ref.shape[1]), F32)


def left_rows(vectors):
    rows = []
    for x in vectors:
        high, low = parts(x)
        rows += [high, high, low]
    return rows


def right_rows(vectors):
    rows = []
    for x in vectors:
        high, low = parts(x)
        rows += [high, low, high]
    return rows


def kernel(
    pools, cons,
    pf_ref, cf_ref, supply_ref, caps_ref, mask_ref, glp_ref, glc_ref,
    pool_out, contract_out,
    kmat, kpeer, pft, pft_in, mask_in, col_part, col_in, mid_part, mid_in,
    row_part, row_in, row_vec, row_vec_in, vee, cbar, left, right,
    pg_part, pg_in, rs_part, rs_in, gathered,
    col_sem, mid_sem, row_sem, vec_sem, feat_sem, mask_sem, pg_sem, rs_sem, agz_sem, agp_sem,
):
    outer = pools // INNER
    me = lax.axis_index("pool")
    con = lax.axis_index("con")
    my_in = lax.rem(me, INNER)
    my_out = me // INNER
    rows = pf_ref.shape[0]
    width = kmat.shape[2]
    feat = pf_ref.shape[1]
    row_tiles = mask_ref.shape[1]
    side = rows // row_tiles

    inner_ids = [(my_out * INNER + lax.rem(my_in + k, INNER), con) for k in range(INNER)]
    outer_ids = [(lax.rem(my_out + k, outer) * INNER + my_in, con) for k in range(outer)]
    con_ids = [(me, lax.rem(con + k, cons)) for k in range(cons)]

    barrier = pltpu.get_barrier_semaphore()
    peers = inner_ids[1:] + outer_ids[1:] + con_ids[1:]
    for peer in peers:
        pl.semaphore_signal(barrier, inc=1, device_id=peer, device_id_type=MESH)

    pending = []

    def send(src, dst, sems, at, peer):
        copy = pltpu.make_async_remote_copy(
            src_ref=src, dst_ref=dst, send_sem=sems.at[(0,) + at], recv_sem=sems.at[(1,) + at],
            device_id=peer, device_id_type=MESH,
        )
        copy.start()
        pending.append(copy)
        return copy

    def kernel_block(dst, feat_rows, feat_cols, mask_of):
        for tile in range(row_tiles):
            at = slice(tile * side, (tile + 1) * side)
            scores = dot(feat_rows(at), feat_cols, NT)
            dst[at, :] = (jnp.exp2(scores * (SCALE * math.log2(math.e))) * mask_of(tile)).astype(BF16)

    def own_block(j, carry):
        kernel_block(
            kmat.at[j], lambda at: pf_ref[at, :], cf_ref[j], lambda tile: mask_ref[j, tile : tile + 1, :]
        )
        return carry

    lax.fori_loop(0, INNER, own_block, 0)
    pft[...] = pf_ref[...].astype(F32).T

    def column_sums(weights, step):
        lhs = split_rows(weights)

        def body(j, carry):
            out = dot(lhs, kmat[j], NN)
            col_part[step, j] = out[0:1] + out[1:2]
            return carry

        lax.fori_loop(0, INNER, body, 0)

    def row_sums(vec):
        def body(j, total):
            return total + dot(split_rows(vec[j]), kmat[j], NT)

        total = lax.fori_loop(0, INNER, body, jnp.zeros((8, rows), F32))
        return total[0:1] + total[1:2]

    def reduce_columns(step, after_inner=None, between=None):
        copies = [
            send(col_part.at[step], col_in.at[step, k - 1], col_sem, (step, k - 1), inner_ids[k])
            for k in range(1, INNER)
        ]
        if between is not None:
            between()
        for copy in copies:
            copy.wait_recv()
        total = col_part[step]
        for k in range(INNER - 1):
            total = total + col_in[step, k]
        mid_part[step] = total
        copies = [
            send(mid_part.at[step], mid_in.at[step, k - 1], mid_sem, (step, k - 1), outer_ids[k])
            for k in range(1, outer)
        ]
        if after_inner is not None:
            after_inner()
        for copy in copies:
            copy.wait_recv()
        for k in range(outer - 1):
            total = total + mid_in[step, k]
        return total

    def reduce_rows(step, part):
        row_part[step] = part
        copies = [
            send(row_part.at[step], row_in.at[step, k - 1], row_sem, (step, k - 1), con_ids[k])
            for k in range(1, cons)
        ]
        for copy in copies:
            copy.wait_recv()
        for k in range(cons - 1):
            part = part + row_in[step, k]
        return part

    vec_copies = []

    def share_rows(which, value):
        row_vec[which] = value
        for k in range(1, INNER):
            vec_copies.append(
                send(row_vec.at[which], row_vec_in.at[k - 1, which], vec_sem, (which, k - 1), inner_ids[k])
            )

    feat_copies = []

    def share_features():
        for k in range(1, INNER):
            feat_copies.append(send(pft, pft_in.at[k - 1], feat_sem, (k - 1,), inner_ids[k]))
            feat_copies.append(
                send(
                    mask_ref.at[lax.rem(my_in + k, INNER)], mask_in.at[k - 1], mask_sem, (k - 1,), inner_ids[k]
                )
            )

    def peer_blocks():
        for copy in feat_copies:
            copy.wait_recv()
        for k in range(INNER - 1):
            rows_k = pft_in[k].T.astype(BF16)
            kernel_block(
                kpeer.at[k], lambda at: rows_k[at, :], cf_ref[my_in],
                lambda tile: mask_in[k, tile : tile + 1, :],
            )

    demand = caps_ref[...].astype(F32)
    supply = supply_ref[...]
    ones = jnp.ones((1, rows), F32)

    column_sums(ones, 0)
    pl.semaphore_wait(barrier, len(peers))
    vee[0] = demand / reduce_columns(0, after_inner=share_features)
    r1 = reduce_rows(0, row_sums(vee.at[0]))
    u1 = supply / r1
    share_rows(0, u1)
    column_sums(u1, 1)
    vee[1] = demand / reduce_columns(1, between=peer_blocks)
    r2 = reduce_rows(1, row_sums(vee.at[1]))
    rbar2 = -glp_ref[...] / r2
    share_rows(1, rbar2)
    column_sums(rbar2, 2)
    s2 = reduce_columns(2)
    v2 = vee[1]
    cbar[1] = -(glc_ref[...] / v2 + s2) * v2 * v2 / demand
    ubar = reduce_rows(2, row_sums(cbar.at[1]))
    rbar1 = -ubar * u1 / r1
    share_rows(2, rbar1)
    column_sums(rbar1, 3)

    def build_left():
        for copy in vec_copies:
            copy.wait_recv()
        fill_rows(left.at[0], left_rows([rbar2, u1, rbar1, ones]))
        for k in range(1, INNER):
            fill_rows(
                left.at[k],
                left_rows([row_vec_in[k - 1, 1], row_vec_in[k - 1, 0], row_vec_in[k - 1, 2], ones]),
            )

    s1 = reduce_columns(3, after_inner=build_left)
    v1 = vee[0]
    cbar[0] = -s1 * v1 * v1 / demand

    for j in range(INNER):
        fill_rows(right.at[j], right_rows([vee[1, j], cbar[1, j], vee[0, j], cbar[0, j]]))

    rhs = right[my_in].astype(BF16)
    weights = dot(left[0].astype(BF16), rhs, TN)
    grad = (kmat[my_in].astype(F32) * weights).astype(BF16)
    total = dot(pft[...].astype(BF16), grad, NN)

    def peer_grad(k, total):
        weights = dot(left[k + 1].astype(BF16), rhs, TN)
        grad = (kpeer[k].astype(F32) * weights).astype(BF16)
        return total + dot(pft_in[k].astype(BF16), grad, NN)

    total = lax.fori_loop(0, INNER - 1, peer_grad, total) * SCALE
    share = feat // outer
    for o in range(outer):
        rs_part[o] = total[o * share : (o + 1) * share]
    rs_copies = [
        send(rs_part.at[lax.rem(my_out + k, outer)], rs_in.at[k - 1], rs_sem, (k - 1,), outer_ids[k])
        for k in range(1, outer)
    ]

    lhs = left[0].astype(BF16)

    def pool_grad_part(j, total):
        weights = dot(lhs, right[j].astype(BF16), TN)
        grad = (kmat[j].astype(F32) * weights).astype(BF16)
        return total + dot(grad, cf_ref[j], NN)

    pg = lax.fori_loop(0, INNER, pool_grad_part, jnp.zeros((rows, feat), F32)) * SCALE
    pg_part[...] = pg
    pg_copies = [
        send(pg_part, pg_in.at[k - 1], pg_sem, (k - 1,), con_ids[k]) for k in range(1, cons)
    ]

    for copy in rs_copies:
        copy.wait_recv()
    mine = rs_part[my_out]
    for k in range(outer - 1):
        mine = mine + rs_in[k]
    gathered[my_in, my_out] = mine
    z_copies = []
    plane_copies = [[] for _ in range(INNER)]

    def spread(slot, k):
        for other in range(1, INNER):
            plane_copies[other].append(send(slot, slot, agp_sem, (k, other - 1), inner_ids[other]))

    slot = gathered.at[my_in, my_out]
    for k in range(1, outer):
        z_copies.append(send(slot, slot, agz_sem, (k - 1,), outer_ids[k]))
    spread(slot, 0)
    for k in range(1, outer):
        z_copies[k - 1].wait_recv()
        spread(gathered.at[my_in, lax.rem(my_out + outer - k, outer)], k)

    for copy in pg_copies:
        copy.wait_recv()
    pg = pg_part[...]
    for k in range(cons - 1):
        pg = pg + pg_in[k]
    pool_out[...] = pg

    def put_out(index):
        block = jnp.concatenate([gathered[index, o] for o in range(outer)], axis=0)
        contract_out[pl.ds(pl.multiple_of(index * width, width), width), :] = block.T

    put_out(my_in)
    for other in range(1, INNER):
        for copy in plane_copies[other]:
            copy.wait_recv()
        put_out(lax.rem(my_in + INNER - other, INNER))
    for copy in pending:
        copy.wait_send()


def shards(pools, cons, pool_feat, contract_feat, supply, caps, eligible, grad_log_pool, grad_log_contract):
    rows, feat = pool_feat.shape
    cols = contract_feat.shape[0]
    outer = pools // INNER
    width = cols // INNER
    row_tiles, col_tiles = eligible.shape
    mask = eligible.astype(F32)
    mask = jnp.repeat(mask, cols // col_tiles, axis=1).reshape(row_tiles, INNER, width).transpose(1, 0, 2)
    share = feat // outer
    vmem = pl.BlockSpec(memory_space=pltpu.VMEM)
    dma = pltpu.SemaphoreType.DMA
    return pl.pallas_call(
        functools.partial(kernel, pools, cons),
        out_shape=(
            jax.ShapeDtypeStruct((rows, feat), F32),
            jax.ShapeDtypeStruct((cols, feat), F32),
        ),
        in_specs=[vmem] * 7,
        out_specs=(vmem, vmem),
        scratch_shapes=[
            pltpu.VMEM((INNER, rows, width), BF16),
            pltpu.VMEM((INNER - 1, rows, width), BF16),
            pltpu.VMEM((feat, rows), F32),
            pltpu.VMEM((INNER - 1, feat, rows), F32),
            pltpu.VMEM((INNER - 1, row_tiles, width), F32),
            pltpu.VMEM((4, INNER, 1, width), F32),
            pltpu.VMEM((4, INNER - 1, INNER, 1, width), F32),
            pltpu.VMEM((4, INNER, 1, width), F32),
            pltpu.VMEM((4, outer - 1, INNER, 1, width), F32),
            pltpu.VMEM((3, 1, rows), F32),
            pltpu.VMEM((3, cons - 1, 1, rows), F32),
            pltpu.VMEM((3, 1, rows), F32),
            pltpu.VMEM((INNER - 1, 3, 1, rows), F32),
            pltpu.VMEM((2, INNER, 1, width), F32),
            pltpu.VMEM((2, INNER, 1, width), F32),
            pltpu.VMEM((INNER, 16, rows), F32),
            pltpu.VMEM((INNER, 16, width), F32),
            pltpu.VMEM((rows, feat), F32),
            pltpu.VMEM((cons - 1, rows, feat), F32),
            pltpu.VMEM((outer, share, width), F32),
            pltpu.VMEM((outer - 1, share, width), F32),
            pltpu.VMEM((INNER, outer, share, width), F32),
            dma((2, 4, INNER - 1)),
            dma((2, 4, outer - 1)),
            dma((2, 3, cons - 1)),
            dma((2, 3, INNER - 1)),
            dma((2, INNER - 1)),
            dma((2, INNER - 1)),
            dma((2, cons - 1)),
            dma((2, outer - 1)),
            dma((2, outer - 1)),
            dma((2, outer, INNER - 1)),
        ],
        compiler_params=pltpu.CompilerParams(
            collective_id=0, has_side_effects=True, vmem_limit_bytes=56 * 1024 * 1024
        ),
        name="sinkhorn",
    )(
        pool_feat,
        contract_feat.reshape(INNER, width, feat),
        supply.reshape(1, rows),
        caps.reshape(INNER, 1, width),
        mask,
        grad_log_pool.reshape(1, rows),
        grad_log_contract.reshape(INNER, 1, width),
    )


def solution(mesh):
    placed = (
        P("pool", None),
        P("con", None),
        P("pool"),
        P("con"),
        P("pool", "con"),
        P("pool"),
        P("con"),
    )
    return jax.shard_map(
        functools.partial(shards, mesh.shape["pool"], mesh.shape["con"]),
        mesh=mesh,
        in_specs=placed,
        out_specs=(P("pool", None), P("con", None)),
        check_vma=False,
    )
```
